32 devices in a mesh: dp: 1 (over z), ep: 4 (over y), tp: 8 (over x, core).
Axes of the slice: x: 4, y: 4, z: 1, core: 2. Of those that a mesh axis runs over, the one named last changes fastest.
The devices are a block of a 4x4x8 slice.
Arguments:
- X: bfloat16 [4096, 2048], P(('dp', 'ep', 'tp'))
- idx: int32 [4096, 8], P(('dp', 'ep', 'tp'))
- g: float32 [4096, 8], P(('dp', 'ep', 'tp'))
- W1: bfloat16 [64, 2048, 1024], P('ep', None, 'tp')
- W3: bfloat16 [64, 2048, 1024], P('ep', None, 'tp')
- W2: bfloat16 [64, 1024, 2048], P('ep', 'tp')
Outputs:
- output: bfloat16 [4096, 2048], P(('dp', 'ep', 'tp'))
All inputs are finite; a program needn't handle non-finite values.
Results may differ from the reference program's by a relative error of at most 0.0100285.
Values are sent between devices in bfloat16 or wider.
A program may use at most 768 MiB of HBM per device.

```python
import jax
import jax.numpy as jnp
from jax import lax

D = 2048
F = 1024
E = 64
TOP = 8
T_LOC = 128
NDEV = 32
C = 2 * TOP * T_LOC // E
T = NDEV * T_LOC


def _weights(key, shape, fan):
    def one(k):
        return (jax.random.normal(k, shape, jnp.float32) * fan ** -0.5).astype(jnp.bfloat16)
    return lax.map(one, jax.random.split(key, E))


def setup_inputs(seed: int = 0, part: int = 0) -> dict:
    key = jax.random.PRNGKey(seed)
    kdata, kw = jax.random.split(key)
    kx, kr, kg = jax.random.split(jax.random.fold_in(kdata, part), 3)
    k1, k3, k2 = jax.random.split(kw, 3)
    x = jax.random.normal(kx, (T, D), jnp.float32).astype(jnp.bfloat16)
    expert_rank = jnp.arange(E, dtype=jnp.uint32)
    wait_scale = jnp.uint32(512) - (jnp.uint32(256) * expert_rank) // jnp.uint32(max(E - 1, 1))
    wait_time = (jax.random.bits(jax.random.fold_in(kr, 7), (T, E), jnp.uint32) >> 10) * wait_scale[None, :]
    idx = jnp.argsort(wait_time, axis=1)[:, :TOP].astype(jnp.int32)
    g = jax.random.uniform(kg, (T, TOP), jnp.float32, 0.25, 1.0)
    return {"X": x, "idx": idx, "g": g,
            "W1": _weights(k1, (D, F), D), "W3": _weights(k3, (D, F), D), "W2": _weights(k2, (F, D), F)}


def _slots(ids):
    oh = (ids[:, None] == jnp.arange(E, dtype=jnp.int32)[None, :]).astype(jnp.int32)
    return jnp.sum(oh * (jnp.cumsum(oh, axis=0) - 1), axis=1)


def reference(X, idx, g, W1, W3, W2):
    ids = idx.reshape(NDEV, T_LOC * TOP)
    s = jax.vmap(_slots)(ids)
    keep = s < C
    dest = jnp.where(keep, ids * C + s, E * C)
    xr = jnp.repeat(X.reshape(NDEV, T_LOC, D), TOP, axis=1)
    buf = jax.vmap(lambda x, dd: jnp.zeros((E * C, D), X.dtype).at[dd].set(x, mode="drop"))(xr, dest)
    buf = buf.reshape(NDEV, E, C, D).transpose(1, 0, 2, 3)

    def expert(a):
        xb, w1, w3, w2 = a

        def rows(x):
            h1 = jnp.dot(x, w1, preferred_element_type=jnp.float32)
            h3 = jnp.dot(x, w3, preferred_element_type=jnp.float32)
            h = (jax.nn.silu(h1) * h3).astype(jnp.bfloat16)
            return jnp.dot(h, w2, preferred_element_type=jnp.float32).astype(jnp.bfloat16)
        return lax.map(rows, xb)

    yb = lax.map(expert, (buf, W1, W3, W2))
    yb = yb.transpose(1, 0, 2, 3).reshape(NDEV, E * C, D)
    ysel = jax.vmap(lambda y, dd: y[jnp.minimum(dd, E * C - 1)])(yb, dest)
    wgt = jnp.where(keep, g.reshape(NDEV, T_LOC * TOP), 0.0)
    out = jnp.sum(ysel.astype(jnp.float32).reshape(NDEV, T_LOC, TOP, D) * wgt.reshape(NDEV, T_LOC, TOP, 1), axis=2)
    return out.reshape(T, D).astype(jnp.bfloat16)
```

```python
import functools

import jax
import jax.numpy as jnp
from jax import lax
from jax.experimental import pallas as pl
from jax.experimental.pallas import tpu as pltpu
from jax.sharding import PartitionSpec as P

CF = 2
RING = 4
MESH = pl.DeviceIdType.MESH
F32, BF16 = jnp.float32, jnp.bfloat16
VMEM_LIMIT = 66 * 1000 * 1000


def _neighbours():
    d, y, t = lax.axis_index("dp"), lax.axis_index("ep"), lax.axis_index("tp")
    x, c = t // 2, t % 2

    def at(dx, dy):
        return (d, (y + dy) % RING, 2 * ((x + dx) % RING) + c)

    pr, pl_ = at(1 - c, c), at(RING - 1 + c, RING - c)
    qr, ql = at(c, 1 - c), at(RING - c, RING - 1 + c)
    return pr, pl_, qr, ql, (d, y, 2 * x + 1 - c)


def _greet(devices):
    barrier = pltpu.get_barrier_semaphore()
    for dev in devices:
        pl.semaphore_signal(barrier, inc=1, device_id=dev, device_id_type=MESH)
    pl.semaphore_wait(barrier, len(devices))


def _up(cap, x, meta, w1, w3, w2, h_out, sg_out, w2x, A, MA, Wt, G, Hb, SG, ssem, rsem, lsem):
    pr, pl_, qr, ql, mate = _neighbours()
    el = w1.shape[0]
    t_loc, d = x.shape
    hf = t_loc // 2
    lo, hi = pl.ds(0, hf), pl.ds(hf, hf)
    gs = el // 4
    fw = w1.shape[2]
    count = [0]

    def remote(src, dst, dev):
        i = count[0]
        count[0] += 1
        return pltpu.make_async_remote_copy(src_ref=src, dst_ref=dst, send_sem=ssem.at[i], recv_sem=rsem.at[i],
                                            device_id=dev, device_id_type=MESH)

    sent = []

    def go(*copies):
        for cp in copies:
            cp.start()
            sent.append(cp)

    lcount = [0]

    def local(src, dst):
        i = lcount[0]
        lcount[0] += 1
        cp = pltpu.make_async_copy(src, dst, lsem.at[i])
        cp.start()
        return cp

    _greet((pr, pl_, qr, ql, mate))

    own_x = local(x, A.at[0, 0])
    own_m = local(meta, MA.at[0, 0])
    r_m, l_m = remote(meta, MA.at[0, 3], pr), remote(meta, MA.at[0, 1], pl_)
    r_lo, r_hi = remote(x.at[lo], A.at[0, 3, lo], pr), remote(x.at[hi], A.at[0, 3, hi], pr)
    l_hi, l_lo = remote(x.at[hi], A.at[0, 1, hi], pl_), remote(x.at[lo], A.at[0, 1, lo], pl_)
    go(r_m, l_m, r_lo, l_hi, r_hi, l_lo)

    own_w, mate_w = [], []
    for g in range(4):
        es = pl.ds(g * gs, gs)
        own_w.append((local(w1.at[es], Wt.at[es, 0, :, pl.ds(0, fw)]), local(w3.at[es], Wt.at[es, 0, :, pl.ds(fw, fw)])))
    for g in range(4):
        es = pl.ds(g * gs, gs)
        pair = (remote(w1.at[es], Wt.at[es, 1, :, pl.ds(0, fw)], mate), remote(w3.at[es], Wt.at[es, 1, :, pl.ds(fw, fw)], mate))
        go(*pair)
        mate_w.append(pair)
    w2_cp = remote(w2, w2x, mate)
    go(w2_cp)

    f_lo, f_hi = remote(A.at[0, 3, lo], A.at[0, 2, lo], pr), remote(A.at[0, 1, hi], A.at[0, 2, hi], pl_)
    f_m = remote(MA.at[0, 3], MA.at[0, 2], pr)
    r_m.wait_recv()
    go(f_m)
    r_lo.wait_recv()
    go(f_lo)
    l_hi.wait_recv()
    go(f_hi)

    qR = [remote(x if i == 0 else A.at[0, i], A.at[3, i], qr) for i in range(4)]
    qL = [remote(x if i == 0 else A.at[0, i], A.at[1, i], ql) for i in range(4)]
    fR = [remote(A.at[3, i, lo], A.at[2, i, lo], qr) for i in range(4)]
    fL = [remote(A.at[1, i, hi], A.at[2, i, hi], ql) for i in range(4)]
    mR, mL, mF = remote(MA.at[0], MA.at[3], qr), remote(MA.at[0], MA.at[1], ql), remote(MA.at[3], MA.at[2], qr)

    go(qR[0], qL[0])
    l_m.wait_recv()
    l_lo.wait_recv()
    go(qR[1], qL[1])
    r_hi.wait_recv()
    go(qR[3], qL[3])
    f_m.wait_recv()
    own_m.wait()
    go(mR, mL)
    f_lo.wait_recv()
    f_hi.wait_recv()
    go(qR[2], qL[2])
    own_x.wait()

    first = (lax.axis_index("ep") * el).astype(F32)
    eid = lax.broadcasted_iota(jnp.int32, (el, t_loc), 0).astype(F32) + first
    tri = (lax.broadcasted_iota(jnp.int32, (t_loc, t_loc), 0)
           < lax.broadcasted_iota(jnp.int32, (t_loc, t_loc), 1)).astype(F32).astype(BF16)
    slot_no = lax.broadcasted_iota(jnp.int32, (cap, t_loc), 0).astype(F32)
    top = meta.shape[0] // 2

    def gather(block):
        def body(i, _):
            b = block(i)
            m = MA.at[b // 4, b % 4]
            hold = jnp.zeros((el, t_loc), F32)
            gate = jnp.zeros((el, t_loc), F32)
            for j in range(top):
                hit = jnp.broadcast_to(m[j:j + 1, :], (el, t_loc)) == eid
                hold = hold + jnp.where(hit, 1.0, 0.0)
                gate = gate + jnp.where(hit, jnp.broadcast_to(m[top + j:top + j + 1, :], (el, t_loc)), 0.0)
            slot = jnp.dot(hold.astype(BF16), tri, preferred_element_type=F32)
            keep = (hold > 0.5) & (slot < cap)
            slot = jnp.where(keep, slot, -1.0)
            SG[b, 0:el, :] = slot
            SG[b, el:2 * el, :] = jnp.where(keep, gate, 0.0)
            pick = jnp.concatenate(
                [jnp.where(jnp.broadcast_to(slot[e:e + 1, :], (cap, t_loc)) == slot_no, 1.0, 0.0) for e in range(el)], axis=0
            ).astype(BF16)
            at = pl.ds(pl.multiple_of(i * cap, cap), cap)
            for n in range(d // 256):
                cols = pl.ds(n * 256, 256)
                rows = jnp.dot(pick, A[b // 4, b % 4, :, cols], preferred_element_type=F32).astype(BF16)
                G[:, at, cols] = rows.reshape(el, cap, 256)
            return 0
        lax.fori_loop(0, 4, body, 0)

    def up(e0, e1, s, blocks):
        def one(e):
            o = jnp.dot(G[e], Wt[e, s], preferred_element_type=F32)
            a, b = o[:, :fw], o[:, fw:]
            h = (jax.nn.silu(a) * b).astype(BF16)
            for i, (dq, dp) in enumerate(blocks):
                Hb[dp, e, dq * cap:(dq + 1) * cap, s * fw:(s + 1) * fw] = h[i * cap:(i + 1) * cap]

        def body(k, _):
            for u in range(4):
                one(e0 + k * 4 + u)
            return 0
        lax.fori_loop(0, (e1 - e0) // 4, body, 0)

    gather(lambda i: i)
    blocks = [(0, i) for i in range(4)]
    for g in range(4):
        for cp in own_w[g]:
            cp.wait()
    up(0, el, 0, blocks)
    for g in range(4):
        for cp in mate_w[g]:
            cp.wait_recv()
        up(g * gs, (g + 1) * gs, 1, blocks)

    mR.wait_recv()
    go(mF)
    mL.wait_recv()
    for i in (0, 1):
        qR[i].wait_recv()
        qL[i].wait_recv()
        go(fR[i], fL[i])
    gather(lambda i: 12 - 8 * (i // 2) + i % 2)
    blocks = [(3, 0), (3, 1), (1, 0), (1, 1)]
    up(0, el, 0, blocks)
    up(0, el, 1, blocks)

    for i in (3, 2):
        qR[i].wait_recv()
        qL[i].wait_recv()
        go(fR[i], fL[i])
    gather(lambda i: 14 - 8 * (i // 2) + i % 2)
    blocks = [(3, 2), (3, 3), (1, 2), (1, 3)]
    up(0, el, 0, blocks)
    up(0, el, 1, blocks)

    mF.wait_recv()
    for i in range(4):
        fR[i].wait_recv()
        fL[i].wait_recv()
    gather(lambda i: 8 + i)
    sg_cp = local(SG, sg_out)
    blocks = [(2, i) for i in range(4)]
    up(0, el, 0, blocks)
    up(0, el, 1, blocks)
    h_cp = local(Hb, h_out)
    w2_cp.wait_recv()
    for cp in sent:
        cp.wait_send()
    sg_cp.wait()
    h_cp.wait()


def _down(cap, h_in, sg_in, w2, w2x, o_ref, W2f, Hv, YP, SG, C3, sF, sR, sL, S0, K1, K3, FR, FL, RL, RR,
          bF, bR, bL, T0, T1, T3, bFR, bFL, bRL, bRR, ssem, rsem, lsem):
    pr, pl_, qr, ql, mate = _neighbours()
    el, fw, d = w2.shape
    t_loc = o_ref.shape[0]
    hf = t_loc // 2
    lo, hi = pl.ds(0, hf), pl.ds(hf, hf)
    gs = el // 4
    count, lcount = [0], [0]
    sent = []

    def remote(src, dst, dev):
        i = count[0]
        count[0] += 1
        return pltpu.make_async_remote_copy(src_ref=src, dst_ref=dst, send_sem=ssem.at[i], recv_sem=rsem.at[i],
                                            device_id=dev, device_id_type=MESH)

    def go(*copies):
        for cp in copies:
            cp.start()
            sent.append(cp)

    def local(src, dst):
        i = lcount[0]
        lcount[0] += 1
        cp = pltpu.make_async_copy(src, dst, lsem.at[i])
        cp.start()
        return cp

    order = (2, 1, 3, 0)
    sg_cp = local(sg_in, SG)
    h_cp = {order[0]: local(h_in.at[order[0]], Hv.at[order[0]])}
    w_cp = []
    for g in range(4):
        es = pl.ds(g * gs, gs)
        w_cp.append((local(w2.at[es], W2f.at[es, pl.ds(0, fw)]), local(w2x.at[es], W2f.at[es, pl.ds(fw, fw)])))
    for dp in order[1:]:
        h_cp[dp] = local(h_in.at[dp], Hv.at[dp])
    _greet((pr, pl_, qr, ql, mate))

    far_r = [remote(sF.at[i, lo], FR.at[i], qr) for i in range(4)]
    far_l = [remote(sF.at[i, hi], FL.at[i], ql) for i in range(4)]
    near_r = [(remote(sR.at[i, lo], RL.at[i, lo], qr), remote(sR.at[i, hi], RL.at[i, hi], qr)) for i in range(4)]
    near_l = [(remote(sL.at[i, lo], RR.at[i, lo], ql), remote(sL.at[i, hi], RR.at[i, hi], ql)) for i in range(4)]
    b_far_r, b_far_l = remote(bF.at[lo], bFR, pr), remote(bF.at[hi], bFL, pl_)
    b_near_r = (remote(bR.at[lo], bRL.at[lo], pr), remote(bR.at[hi], bRL.at[hi], pr))
    b_near_l = (remote(bL.at[lo], bRR.at[lo], pl_), remote(bL.at[hi], bRR.at[hi], pl_))

    ncol = el * cap
    row_no = lax.broadcasted_iota(jnp.int32, (4 * el, ncol), 0)
    col_e = lax.broadcasted_iota(jnp.int32, (4 * el, ncol), 1) // cap
    spread = [jnp.where(row_no == col_e + k * el, 1.0, 0.0).astype(BF16) for k in range(4)]
    col_s = (lax.broadcasted_iota(jnp.int32, (t_loc, ncol), 1) % cap).astype(F32)

    def down(dp, e0, e1):
        def one(e):
            for n in range(d // 256):
                cols = pl.ds(n * 256, 256)
                y = jnp.dot(Hv[dp, e], W2f[e, :, cols], preferred_element_type=F32).astype(BF16)
                YP[:, pl.ds(pl.multiple_of(e * cap, cap), cap), cols] = y.reshape(4, cap, 256)

        def body(k, _):
            for u in range(2):
                one(e0 + k * 2 + u)
            return 0
        lax.fori_loop(0, (e1 - e0) // 2, body, 0)

    def combine(dp, dq, put):
        b = dq * 4 + dp
        gate = SG[b, el:2 * el, :]
        g1 = gate.astype(BF16).astype(F32)
        g2 = (gate - g1).astype(BF16).astype(F32)
        g3 = gate - g1 - g2
        table = jnp.concatenate([SG[b, 0:el, :], g1, g2, g3], axis=0).T.astype(BF16)
        slot = jnp.dot(table, spread[0], preferred_element_type=F32)
        hit = slot == col_s
        for k in range(3):
            piece = jnp.dot(table, spread[k + 1], preferred_element_type=F32)
            C3[k * t_loc:(k + 1) * t_loc, :] = jnp.where(hit, piece, 0.0).astype(BF16)
        for n in range(d // 256):
            cols = pl.ds(n * 256, 256)
            z = jnp.dot(C3[...], YP[dq, :, cols], preferred_element_type=F32)
            put(z[:t_loc] + z[t_loc:2 * t_loc] + z[2 * t_loc:], cols)

    def put_far(dp):
        def put(z, cols):
            sF[dp, :, cols] = z.astype(BF16)
        return put

    def put_right(dp):
        def put(z, cols):
            K1[dp, :, cols] = z[:hf]
            sR[dp, hi, cols] = z[hf:].astype(BF16)
        return put

    def put_left(dp):
        def put(z, cols):
            K3[dp, :, cols] = z[hf:]
            sL[dp, lo, cols] = z[:hf].astype(BF16)
        return put

    def put_own(dp):
        def put(z, cols):
            S0[dp, :, cols] = z
        return put

    def pass_on(dp):
        far_r[dp].wait_recv()
        sR[dp, lo, :] = (K1[dp] + FR[dp].astype(F32)).astype(BF16)
        go(near_r[dp][0])
        far_l[dp].wait_recv()
        sL[dp, hi, :] = (K3[dp] + FL[dp].astype(F32)).astype(BF16)
        go(near_l[dp][1])

    def finish(dp):
        for cp in near_r[dp] + near_l[dp]:
            cp.wait_recv()

        def total(rows):
            return S0[dp, rows, :] + RL[dp, rows, :].astype(F32) + RR[dp, rows, :].astype(F32)
        if dp == 2:
            bF[lo, :] = total(lo).astype(BF16)
            go(b_far_r)
            bF[hi, :] = total(hi).astype(BF16)
            go(b_far_l)
        elif dp == 1:
            bR[hi, :] = total(hi).astype(BF16)
            go(b_near_r[1])
            T1[...] = total(lo)
        elif dp == 3:
            bL[lo, :] = total(lo).astype(BF16)
            go(b_near_l[0])
            T3[...] = total(hi)
        else:
            T0[lo, :] = total(lo)
            T0[hi, :] = total(hi)

    sg_cp.wait()
    for k, dp in enumerate(order):
        h_cp[dp].wait()
        if k == 0:
            for g in range(4):
                for cp in w_cp[g]:
                    cp.wait()
                down(dp, g * gs, (g + 1) * gs)
        else:
            down(dp, 0, el)
        if k >= 1:
            pass_on(order[k - 1])
        if k >= 2:
            finish(order[k - 2])
        combine(dp, 2, put_far(dp))
        go(far_r[dp], far_l[dp])
        combine(dp, 1, put_right(dp))
        go(near_r[dp][1])
        combine(dp, 3, put_left(dp))
        go(near_l[dp][0])
        combine(dp, 0, put_own(dp))
    pass_on(0)
    b_far_r.wait_recv()
    bR[lo, :] = (T1[...] + bFR[...].astype(F32)).astype(BF16)
    go(b_near_r[0])
    finish(3)
    b_far_l.wait_recv()
    bL[hi, :] = (T3[...] + bFL[...].astype(F32)).astype(BF16)
    go(b_near_l[1])
    finish(0)
    for cp in b_near_r + b_near_l:
        cp.wait_recv()
    o_ref[...] = (T0[...] + bRL[...].astype(F32) + bRR[...].astype(F32)).astype(BF16)
    for cp in sent:
        cp.wait_send()


def _local(mesh, x, idx, g, w1, w3, w2):
    t_loc, d = x.shape
    top = idx.shape[1]
    el, _, fw = w1.shape
    n_exp = el * mesh.shape["ep"]
    cap = CF * top * t_loc // n_exp
    hf = t_loc // 2
    meta = jnp.concatenate([idx.T.astype(F32), g.T], axis=0)
    hbm = pl.BlockSpec(memory_space=pl.ANY)
    vmem = pl.BlockSpec(memory_space=pltpu.VMEM)
    sems = pltpu.SemaphoreType.DMA
    h, sg, w2x = pl.pallas_call(
        functools.partial(_up, cap),
        out_shape=(jax.ShapeDtypeStruct((4, el, 4 * cap, 2 * fw), BF16),
                   jax.ShapeDtypeStruct((16, 2 * el, t_loc), F32),
                   jax.ShapeDtypeStruct(w2.shape, BF16)),
        in_specs=[hbm] * 5,
        out_specs=(hbm, hbm, hbm),
        scratch_shapes=[
            pltpu.VMEM((4, 4, t_loc, d), BF16),
            pltpu.VMEM((4, 4, 2 * top, t_loc), F32),
            pltpu.VMEM((el, 2, d, 2 * fw), BF16),
            pltpu.VMEM((el, 4 * cap, d), BF16),
            pltpu.VMEM((4, el, 4 * cap, 2 * fw), BF16),
            pltpu.VMEM((16, 2 * el, t_loc), F32),
            sems((40,)), sems((40,)), sems((16,)),
        ],
        compiler_params=pltpu.CompilerParams(collective_id=0, has_side_effects=True, vmem_limit_bytes=VMEM_LIMIT),
    )(x, meta, w1, w3, w2)
    half, full = (hf, d), (t_loc, d)
    return pl.pallas_call(
        functools.partial(_down, cap),
        out_shape=jax.ShapeDtypeStruct((t_loc, d), BF16),
        in_specs=[hbm] * 4,
        out_specs=vmem,
        scratch_shapes=[
            pltpu.VMEM((el, 2 * fw, d), BF16),
            pltpu.VMEM((4, el, 4 * cap, 2 * fw), BF16),
            pltpu.VMEM((4, el * cap, d), BF16),
            pltpu.VMEM((16, 2 * el, t_loc), F32),
            pltpu.VMEM((3 * t_loc, el * cap), BF16),
            pltpu.VMEM((4,) + full, BF16), pltpu.VMEM((4,) + full, BF16), pltpu.VMEM((4,) + full, BF16),
            pltpu.VMEM((4,) + full, F32), pltpu.VMEM((4,) + half, F32), pltpu.VMEM((4,) + half, F32),
            pltpu.VMEM((4,) + half, BF16), pltpu.VMEM((4,) + half, BF16),
            pltpu.VMEM((4,) + full, BF16), pltpu.VMEM((4,) + full, BF16),
            pltpu.VMEM(full, BF16), pltpu.VMEM(full, BF16), pltpu.VMEM(full, BF16),
            pltpu.VMEM(full, F32), pltpu.VMEM(half, F32), pltpu.VMEM(half, F32),
            pltpu.VMEM(half, BF16), pltpu.VMEM(half, BF16), pltpu.VMEM(full, BF16), pltpu.VMEM(full, BF16),
            sems((40,)), sems((40,)), sems((16,)),
        ],
        compiler_params=pltpu.CompilerParams(collective_id=1, has_side_effects=True, vmem_limit_bytes=VMEM_LIMIT),
    )(h, sg, w2, w2x)


def solution(mesh):
    rows = P(("dp", "ep", "tp"), None)
    return jax.shard_map(functools.partial(_local, mesh), mesh=mesh,
                         in_specs=(rows, rows, rows, P("ep", None, "tp"), P("ep", None, "tp"), P("ep", "tp", None)),
                         out_specs=rows, check_vma=False)
```

```python
import functools

import jax
import jax.numpy as jnp
from jax import lax
from jax.experimental import pallas as pl
from jax.experimental.pallas import tpu as pltpu
from jax.sharding import PartitionSpec as P

CF = 2
RING = 4
MESH = pl.DeviceIdType.MESH
F32, BF16 = jnp.float32, jnp.bfloat16
VMEM_LIMIT = 67043328
GATHER_UNROLL = 2
UP_UNROLL = 8


def _neighbours():
    d, y, t = lax.axis_index("dp"), lax.axis_index("ep"), lax.axis_index("tp")
    x, c = t // 2, t % 2

    def at(dx, dy):
        return (d, (y + dy) % RING, 2 * ((x + dx) % RING) + c)

    pr, pl_ = at(1 - c, c), at(RING - 1 + c, RING - c)
    qr, ql = at(c, 1 - c), at(RING - c, RING - 1 + c)
    return pr, pl_, qr, ql, (d, y, 2 * x + 1 - c)


def _greet(devices):
    barrier = pltpu.get_barrier_semaphore()
    for dev in devices:
        pl.semaphore_signal(barrier, inc=1, device_id=dev, device_id_type=MESH)
    pl.semaphore_wait(barrier, len(devices))


def _layer(cap, x, idx, gate_in, w1, w3, w2, o_out, w2x, A, MA, Wt, G, Hb, SG, C3, FR, FL, RL, RR, bFR, bFL, bRL, bRR,
           ssem, rsem, lsem):
    pr, pl_, qr, ql, mate = _neighbours()
    el, _, fw = w1.shape
    t_loc, d = x.shape
    top = idx.shape[0]
    hf = t_loc // 2
    lo, hi = pl.ds(0, hf), pl.ds(hf, hf)
    gs = el // 4
    count, lcount = [0], [0]
    open_sends = []

    def remote(src, dst, dev):
        i = count[0]
        count[0] += 1
        return pltpu.make_async_remote_copy(src_ref=src, dst_ref=dst, send_sem=ssem.at[i], recv_sem=rsem.at[i],
                                            device_id=dev, device_id_type=MESH)

    def go(*copies):
        for cp in copies:
            cp.start()
            open_sends.append(cp)

    def sent(*copies):
        for cp in copies:
            cp.wait_send()
            open_sends[:] = [o for o in open_sends if o is not cp]

    def local(src, dst):
        i = lcount[0]
        lcount[0] += 1
        cp = pltpu.make_async_copy(src, dst, lsem.at[i])
        cp.start()
        return cp

    own_x = local(x, A.at[0, 0])
    own_w = []
    for g in range(4):
        es = pl.ds(g * gs, gs)
        own_w.append((local(w1.at[es], Wt.at[es, 0, :, pl.ds(0, fw)]), local(w3.at[es], Wt.at[es, 0, :, pl.ds(fw, fw)])))
    MA[0, 0, 0:top, :] = idx[...].astype(F32)
    MA[0, 0, top:2 * top, :] = gate_in[...]
    _greet((pr, pl_, qr, ql, mate))

    r_lo, r_hi = remote(x.at[lo], A.at[0, 3, lo], pr), remote(x.at[hi], A.at[0, 3, hi], pr)
    l_hi, l_lo = remote(x.at[hi], A.at[0, 1, hi], pl_), remote(x.at[lo], A.at[0, 1, lo], pl_)
    r_m, l_m = remote(MA.at[0, 0], MA.at[0, 3], pr), remote(MA.at[0, 0], MA.at[0, 1], pl_)
    go(r_lo, l_hi, r_m, l_m, r_hi, l_lo)
    mate_w = []
    for g in range(4):
        es = pl.ds(g * gs, gs)
        pair = (remote(w1.at[es], Wt.at[es, 1, :, pl.ds(0, fw)], mate), remote(w3.at[es], Wt.at[es, 1, :, pl.ds(fw, fw)], mate))
        go(*pair)
        mate_w.append(pair)
    w2_cp = remote(w2, w2x, mate)
    go(w2_cp)

    f_lo, f_hi = remote(A.at[0, 3, lo], A.at[0, 2, lo], pr), remote(A.at[0, 1, hi], A.at[0, 2, hi], pl_)
    f_m = remote(MA.at[0, 3], MA.at[0, 2], pr)
    r_lo.wait_recv()
    go(f_lo)
    l_hi.wait_recv()
    go(f_hi)
    r_m.wait_recv()
    go(f_m)

    qR = [remote(x if i == 0 else A.at[0, i], A.at[3, i], qr) for i in range(4)]
    qL = [remote(x if i == 0 else A.at[0, i], A.at[1, i], ql) for i in range(4)]
    fR = [remote(A.at[3, i, lo], A.at[2, i, lo], qr) for i in range(4)]
    fL = [remote(A.at[1, i, hi], A.at[2, i, hi], ql) for i in range(4)]
    mR, mL, mF = remote(MA.at[0], MA.at[3], qr), remote(MA.at[0], MA.at[1], ql), remote(MA.at[3], MA.at[2], qr)

    go(qR[0], qL[0])
    l_m.wait_recv()
    l_lo.wait_recv()
    go(qR[1], qL[1])
    r_hi.wait_recv()
    go(qR[3], qL[3])
    f_m.wait_recv()
    go(mR, mL)
    f_lo.wait_recv()
    f_hi.wait_recv()
    go(qR[2], qL[2])
    own_x.wait()

    far_r = [remote(A.at[2, i, lo], FR.at[i], qr) for i in range(4)]
    far_l = [remote(A.at[2, i, hi], FL.at[i], ql) for i in range(4)]
    near_r = [(remote(A.at[1, i, lo], RL.at[i, lo], qr), remote(A.at[1, i, hi], RL.at[i, hi], qr)) for i in range(4)]
    near_l = [(remote(A.at[3, i, lo], RR.at[i, lo], ql), remote(A.at[3, i, hi], RR.at[i, hi], ql)) for i in range(4)]
    b_far_r, b_far_l = remote(A.at[0, 2, lo], bFR, pr), remote(A.at[0, 2, hi], bFL, pl_)
    b_near_r = (remote(A.at[0, 1, lo], bRL.at[lo], pr), remote(A.at[0, 1, hi], bRL.at[hi], pr))
    b_near_l = (remote(A.at[0, 3, lo], bRR.at[lo], pl_), remote(A.at[0, 3, hi], bRR.at[hi], pl_))

    first = (lax.axis_index("ep") * el).astype(F32)
    eid = lax.broadcasted_iota(jnp.int32, (el, t_loc), 0).astype(F32) + first
    tri = (lax.broadcasted_iota(jnp.int32, (t_loc, t_loc), 0)
           < lax.broadcasted_iota(jnp.int32, (t_loc, t_loc), 1)).astype(F32).astype(BF16)
    slot_no = lax.broadcasted_iota(jnp.int32, (cap, t_loc), 0).astype(F32)
    ncol = el * cap
    row_no = lax.broadcasted_iota(jnp.int32, (4 * el, ncol), 0)
    col_e = lax.broadcasted_iota(jnp.int32, (4 * el, ncol), 1) // cap
    spread = [jnp.where(row_no == col_e + k * el, 1.0, 0.0).astype(BF16) for k in range(4)]
    col_s = (lax.broadcasted_iota(jnp.int32, (t_loc, ncol), 1) % cap).astype(F32)

    def gather(block, i0=0, i1=4):
        def one(i):
            b = block(i)
            m = MA.at[b // 4, b % 4]
            hold = jnp.zeros((el, t_loc), F32)
            gate = jnp.zeros((el, t_loc), F32)
            for j in range(top):
                hit = jnp.broadcast_to(m[j:j + 1, :], (el, t_loc)) == eid
                hold = hold + jnp.where(hit, 1.0, 0.0)
                gate = gate + jnp.where(hit, jnp.broadcast_to(m[top + j:top + j + 1, :], (el, t_loc)), 0.0)
            slot = jnp.dot(hold.astype(BF16), tri, preferred_element_type=F32)
            keep = (hold > 0.5) & (slot < cap)
            slot = jnp.where(keep, slot, -1.0)
            SG[b, 0:el, :] = slot
            SG[b, el:2 * el, :] = jnp.where(keep, gate, 0.0)
            pick = jnp.concatenate(
                [jnp.where(jnp.broadcast_to(slot[e:e + 1, :], (cap, t_loc)) == slot_no, 1.0, 0.0) for e in range(el)], axis=0
            ).astype(BF16)
            at = pl.ds(pl.multiple_of(i * cap, cap), cap)
            for n in range(d // 256):
                cols = pl.ds(n * 256, 256)
                rows = jnp.dot(pick, A[b // 4, b % 4, :, cols], preferred_element_type=F32).astype(BF16)
                G[:, at, cols] = rows.reshape(el, cap, 256)

        def body(k, _):
            for u in range(GATHER_UNROLL):
                one(k * GATHER_UNROLL + u)
            return 0
        lax.fori_loop(i0 // GATHER_UNROLL, i1 // GATHER_UNROLL, body, 0)

    def up(e0, n, s, hs, unroll):
        def one(e):
            o = jnp.dot(G[e], Wt[e, s], preferred_element_type=F32)
            Hb[hs, e, :, s * fw:(s + 1) * fw] = (jax.nn.silu(o[:, :fw]) * o[:, fw:]).astype(BF16)

        def body(k, _):
            for u in range(unroll):
                one(e0 + k * unroll + u)
            return 0
        lax.fori_loop(0, n // unroll, body, 0)

    def w2_over(g):
        copies = []
        es = pl.ds(g * gs, gs)
        for n in range(d // 256):
            cols = pl.ds(n * 256, 256)
            copies.append(local(w2.at[es, :, cols], Wt.at[es, 0, pl.ds(n * 256, fw), :]))
            copies.append(local(w2x.at[es, :, cols], Wt.at[es, 0, pl.ds(n * 256 + fw, fw), :]))
        return copies

    def down(hs, k0, k1):
        def body(k, _):
            for u in range(4):
                e = k * 4 + u
                for n in range(d // 256):
                    cols = pl.ds(n * 256, 256)
                    y = jnp.dot(Hb[hs, e], Wt[e, 0, cols, :], preferred_element_type=F32).astype(BF16)
                    for i in range(4):
                        G[4 * i + k, u * cap:(u + 1) * cap, cols] = y[i * cap:(i + 1) * cap]
            return 0
        lax.fori_loop(k0, k1, body, 0)

    def combine(i, dq, dp):
        b = dq * 4 + dp
        gate = SG[b, el:2 * el, :]
        g1 = gate.astype(BF16).astype(F32)
        g2 = (gate - g1).astype(BF16).astype(F32)
        g3 = gate - g1 - g2
        table = jnp.concatenate([SG[b, 0:el, :], g1, g2, g3], axis=0).T.astype(BF16)
        slot = jnp.dot(table, spread[0], preferred_element_type=F32)
        hit = slot == col_s
        for k in range(3):
            piece = jnp.dot(table, spread[k + 1], preferred_element_type=F32)
            C3[k * t_loc:(k + 1) * t_loc, :] = jnp.where(hit, piece, 0.0).astype(BF16)
        for n in range(d // 256):
            cols = pl.ds(n * 256, 256)
            z = jnp.dot(C3[...], G[pl.ds(4 * i, 4), :, cols].reshape(ncol, 256), preferred_element_type=F32)
            A[dq, dp, :, cols] = (z[:t_loc] + z[t_loc:2 * t_loc] + z[2 * t_loc:]).astype(BF16)

    def pass_on(dp):
        far_r[dp].wait_recv()
        A[1, dp, lo, :] = (A[1, dp, lo, :].astype(F32) + FR[dp].astype(F32)).astype(BF16)
        go(near_r[dp][0])
        far_l[dp].wait_recv()
        A[3, dp, hi, :] = (A[3, dp, hi, :].astype(F32) + FL[dp].astype(F32)).astype(BF16)
        go(near_l[dp][1])

    def total(dp, rows):
        return A[0, dp, rows, :].astype(F32) + RL[dp, rows, :].astype(F32) + RR[dp, rows, :].astype(F32)

    gather(lambda i: i)
    for g in range(4):
        for cp in own_w[g]:
            cp.wait()
    up(0, el, 0, 0, UP_UNROLL)
    for g in range(4):
        for cp in mate_w[g]:
            cp.wait_recv()
        up(g * gs, gs, 1, 0, gs)

    mR.wait_recv()
    go(mF)
    mL.wait_recv()
    for i in (0, 1):
        qR[i].wait_recv()
        qL[i].wait_recv()
        go(fR[i], fL[i])
    gather(lambda i: 12 - 8 * (i // 2) + i % 2)
    up(0, el, 0, 1, UP_UNROLL)
    up(0, el, 1, 1, UP_UNROLL)

    for i in (3, 2):
        qR[i].wait_recv()
        qL[i].wait_recv()
        go(fR[i], fL[i])
    gather(lambda i: 14 - 8 * (i // 2) + i % 2)
    up(0, el, 0, 2, UP_UNROLL)
    up(0, el, 1, 2, UP_UNROLL)

    mF.wait_recv()
    for i in (0, 1):
        fR[i].wait_recv()
        fL[i].wait_recv()
    gather(lambda i: 8 + i, 0, 2)
    for i in (3, 2):
        fR[i].wait_recv()
        fL[i].wait_recv()
    gather(lambda i: 8 + i, 2, 4)
    w2_cp.wait_recv()
    w2_cps = []
    for g in range(2):
        up(2 * g * gs, 2 * gs, 0, 3, UP_UNROLL)
        w2_cps += [w2_over(2 * g), w2_over(2 * g + 1)]
    up(0, el, 1, 3, UP_UNROLL)
    for k in range(4):
        for cp in w2_cps[k]:
            cp.wait()
        down(3, k, k + 1)
    for dp in (2, 1, 3, 0):
        combine(dp, 2, dp)
        go(far_r[dp], far_l[dp])

    down(2, 0, 4)
    sent(fR[2], fL[2], fR[3], fL[3])
    for i, dp in ((0, 2), (1, 3)):
        combine(i, 3, dp)
        go(near_l[dp][0])
        combine(i + 2, 1, dp)
        go(near_r[dp][1])
    pass_on(2)
    pass_on(3)
    down(1, 0, 4)
    sent(fR[0], fL[0], fR[1], fL[1])

    def chunk1(i, _):
        combine(i, 3, i)
        combine(i + 2, 1, i)
        return 0
    lax.fori_loop(0, 2, chunk1, 0)
    for dp in (1, 0):
        go(near_l[dp][0], near_r[dp][1])
        pass_on(dp)

    down(0, 0, 4)
    sent(*qR, *qL, f_lo, f_hi)
    combine(2, 0, 2)
    for cp in near_r[2] + near_l[2]:
        cp.wait_recv()
    A[0, 2, lo, :] = total(2, lo).astype(BF16)
    go(b_far_r)
    A[0, 2, hi, :] = total(2, hi).astype(BF16)
    go(b_far_l)

    def chunk0(k, _):
        dp = (2 * k + 1) % 5
        combine(dp, 0, dp)
        return 0
    lax.fori_loop(0, 3, chunk0, 0)
    for cp in near_r[1] + near_l[1]:
        cp.wait_recv()
    A[0, 1, hi, :] = total(1, hi).astype(BF16)
    go(b_near_r[1])
    for cp in near_r[3] + near_l[3]:
        cp.wait_recv()
    A[0, 3, lo, :] = total(3, lo).astype(BF16)
    go(b_near_l[0])
    b_far_r.wait_recv()
    A[0, 1, lo, :] = (total(1, lo) + bFR[...].astype(F32)).astype(BF16)
    go(b_near_r[0])
    b_far_l.wait_recv()
    A[0, 3, hi, :] = (total(3, hi) + bFL[...].astype(F32)).astype(BF16)
    go(b_near_l[1])
    for cp in near_r[0] + near_l[0] + b_near_r + b_near_l:
        cp.wait_recv()
    for rows in (lo, hi):
        A[0, 0, rows, :] = (total(0, rows) + bRL[rows, :].astype(F32) + bRR[rows, :].astype(F32)).astype(BF16)
    out_cp = local(A.at[0, 0], o_out)
    for cp in open_sends:
        cp.wait_send()
    out_cp.wait()


def _local(mesh, x, idx, g, w1, w3, w2):
    t_loc, d = x.shape
    top = idx.shape[1]
    el, _, fw = w1.shape
    cap = CF * top * t_loc // (el * mesh.shape["ep"])
    half, full = (t_loc // 2, d), (t_loc, d)
    hbm = pl.BlockSpec(memory_space=pl.ANY)
    vmem = pl.BlockSpec(memory_space=pltpu.VMEM)
    sems = pltpu.SemaphoreType.DMA
    out, _ = pl.pallas_call(
        functools.partial(_layer, cap),
        out_shape=(jax.ShapeDtypeStruct((t_loc, d), BF16), jax.ShapeDtypeStruct(w2.shape, BF16)),
        in_specs=[hbm, vmem, vmem, hbm, hbm, hbm],
        out_specs=(hbm, hbm),
        scratch_shapes=[
            pltpu.VMEM((4, 4) + full, BF16),
            pltpu.VMEM((4, 4, 2 * top, t_loc), F32),
            pltpu.VMEM((el, 2, d, 2 * fw), BF16),
            pltpu.VMEM((el, 4 * cap, d), BF16),
            pltpu.VMEM((4, el, 4 * cap, 2 * fw), BF16),
            pltpu.VMEM((16, 2 * el, t_loc), F32),
            pltpu.VMEM((3 * t_loc, el * cap), BF16),
            pltpu.VMEM((4,) + half, BF16), pltpu.VMEM((4,) + half, BF16),
            pltpu.VMEM((4,) + full, BF16), pltpu.VMEM((4,) + full, BF16),
            pltpu.VMEM(half, BF16), pltpu.VMEM(half, BF16), pltpu.VMEM(full, BF16), pltpu.VMEM(full, BF16),
            sems((80,)), sems((80,)), sems((80,)),
        ],
        compiler_params=pltpu.CompilerParams(collective_id=0, has_side_effects=True, vmem_limit_bytes=VMEM_LIMIT),
    )(x, idx.T, g.T, w1, w3, w2)
    return out


def solution(mesh):
    rows = P(("dp", "ep", "tp"), None)
    return jax.shard_map(functools.partial(_local, mesh), mesh=mesh,
                         in_specs=(rows, rows, rows, P("ep", None, "tp"), P("ep", None, "tp"), P("ep", "tp", None)),
                         out_specs=rows, check_vma=False)
```
